32 devices in a mesh: gx: 2 (over core), gy: 4 (over y, x), gz: 4 (over z).
Axes of the slice: x: 2, y: 2, z: 4, core: 2. Of those that a mesh axis runs over, the one named last changes fastest.
Arguments:
- factors: bfloat16 [6144, 8, 4096], P('gy', None, 'gz'), may hold values from -0.046875 to 0.046875
- trial_vectors: float32 [64, 8, 4096], P('gx', None, 'gz'), may hold values from -6 to 6
- energy_gap: float32 [8, 4096], P(None, 'gz'), may hold values from 0.5 to 4
Outputs:
- updated_vectors: float32 [64, 8, 4096], P('gx', None, 'gz')
- coupling: float32 [64, 64], P(None, 'gx')
The draws below stay inside these ranges and needn't reach their ends.
All inputs are finite; a program needn't handle non-finite values.
Results may differ from the reference program's by a relative error of at most 0.02.
Values may be sent and summed in bfloat16 or wider, within the bound.
A program may use at most 192 MiB of HBM per device.

```python
import math
import jax
import jax.numpy as jnp
from jax import lax

NBAS = 4096
NAUX = 6144
ROWS = 8
ITERS = 2
VECS = 64
N_GZ = 4


def draw_trial_vectors(key, part):
    first_key = jax.random.fold_in(jax.random.fold_in(key, 17), 0)
    base_draw = jnp.clip(jax.random.normal(first_key, (VECS, ROWS, NBAS), jnp.float32), -4.0, 4.0)
    return base_draw


def shard_levels(own_key, dims, cuts, low, top_value):
    factor_of = 1.0
    for position, blocks in cuts:
        steps = jax.random.uniform(jax.random.fold_in(jax.random.fold_in(own_key, 6), position), (blocks,), jnp.float32, low / len(cuts), top_value / len(cuts))
        factor_of = factor_of * jnp.repeat(jnp.exp(steps), dims[position] // blocks).reshape((-1,) + (1,) * (len(dims) - 1 - position))
    return factor_of


def centred(stream_key, dims, deviation, most, cuts=(), held_as=jnp.bfloat16):
    values = deviation * jax.random.normal(stream_key, dims, jnp.float32)
    if cuts:
        values = values * shard_levels(stream_key, dims, cuts, -0.22, 0.18)
    return jnp.clip(values, -most, most).astype(held_as)


def setup_inputs(seed: int = 0) -> dict:
    splits = jax.random.split(jax.random.key(seed), 4)
    return {
        "factors": centred(splits[0], (NAUX, ROWS, NBAS), (4 * NBAS) ** -0.5, 0.046875, ((0, 4), (2, 4))),
        "trial_vectors": draw_trial_vectors(jax.random.fold_in(splits[3], 71), 0),
        "energy_gap": jnp.clip(jnp.exp(math.log(4.0) - 2.0794415 * jax.random.uniform(splits[2], (ROWS, NBAS), jnp.float32) ** shard_levels(splits[2], (ROWS, NBAS), ((1, 4),), -0.2, 0.2)), 0.5, 4.0),
    }


def solve_subspace(gram_matrix, projected):
    lower_factor = jnp.linalg.cholesky(gram_matrix)
    inner_solve = lax.linalg.triangular_solve(lower_factor, projected, left_side=True, lower=True)
    return lax.linalg.triangular_solve(lower_factor, inner_solve, left_side=True, lower=True, transpose_a=True)

def reference(factors, trial_vectors, energy_gap):
    highest = lax.Precision.HIGHEST
    block_width = NBAS // N_GZ
    current = trial_vectors
    coupling = jnp.zeros((VECS, VECS), jnp.float32)
    for iteration in range(ITERS):
        compact = lax.optimization_barrier(current.astype(jnp.bfloat16)).astype(jnp.float32)
        fitted = jnp.zeros((VECS, NAUX), jnp.float32)
        mixed_fit = jnp.zeros((VECS, ROWS, ROWS, NAUX), jnp.float32)
        for column_block in range(N_GZ):
            start = column_block * block_width
            factor_block = factors[:, :, start:start + block_width].astype(jnp.float32)
            compact_block = compact[:, :, start:start + block_width]
            fitted = fitted + jnp.einsum('prn,krn->kp', factor_block, compact_block, precision=highest)
            partial_block = jnp.einsum('prn,kln->klrp', factor_block, compact_block, precision=highest)
            mixed_fit = mixed_fit + lax.optimization_barrier(partial_block.astype(jnp.bfloat16)).astype(jnp.float32)
        fitted_b = lax.optimization_barrier(fitted.astype(jnp.bfloat16)).astype(jnp.float32)
        mixed_b = lax.optimization_barrier(mixed_fit.astype(jnp.bfloat16)).astype(jnp.float32)
        pieces = []
        for column_block in range(N_GZ):
            start = column_block * block_width
            factor_block = factors[:, :, start:start + block_width].astype(jnp.float32)
            coulomb = jnp.einsum('prn,kp->krn', factor_block, fitted_b, precision=highest)
            exchange_part = jnp.einsum('klrp,pln->krn', mixed_b, factor_block, precision=highest)
            pieces.append(2.0 * coulomb - exchange_part)
        fock_part = jnp.concatenate(pieces, axis=2)
        sigma_all = energy_gap[None, :, :] * current + fock_part
        gram_matrix = jnp.einsum('krn,lrn->kl', current, current, precision=highest)
        projected = jnp.einsum('lrn,krn->lk', current, sigma_all, precision=highest)
        coupling = solve_subspace(gram_matrix, projected)
        residual = sigma_all - jnp.einsum('lrn,lk->krn', current, coupling, precision=highest)
        current = current - residual / energy_gap[None, :, :]
    return (current, coupling)
```

```python
import jax
import jax.numpy as jnp
from jax import lax
from jax.sharding import PartitionSpec as P

ITERS = 2
B16 = jnp.bfloat16
F32 = jnp.float32


def ring(size, shift):
    return [(i, (i + shift) % size) for i in range(size)]


def send_z(block, shift, size, axis=1):
    shift = shift % size
    if 2 * shift != size:
        return lax.ppermute(block, "gz", ring(size, shift))
    half = block.shape[axis] // 2
    first, second = lax.split(block, (half, block.shape[axis] - half), axis=axis)
    for part_shift in (1, shift - 1):
        if part_shift:
            first = lax.ppermute(first, "gz", ring(size, part_shift))
            second = lax.ppermute(second, "gz", ring(size, -part_shift))
    return lax.concatenate((first, second), axis)


def move_z(block, shift, size):
    shift = shift % size
    return lax.ppermute(block, "gz", ring(size, shift)) if shift else block


def butterfly(block, size, descending):
    bits = [1 << b for b in range(size.bit_length() - 1)]
    for bit in reversed(bits) if descending else bits:
        other = lax.ppermute(block, "gy", [(i, i ^ bit) for i in range(size)])
        block = (block.astype(F32) + other.astype(F32)).astype(B16)
    return block


def both_groups(block, me, size_x):
    other = lax.ppermute(block, "gx", ring(size_x, 1))
    first = jnp.where(me == 0, block, other)
    second = jnp.where(me == 0, other, block)
    return lax.concatenate((first, second), 1)


def make_per_device(nx, ny, nz):
    order = sorted(range(nz), key=lambda s: min(s, nz - s))

    def per_device(factors, trial_vectors, energy_gap):
        me_x, me_z = lax.axis_index("gx"), lax.axis_index("gz")
        aux, rows, width = factors.shape
        share = aux // (nx * nz)
        cut = factors.reshape(nz, nx, share, rows, width)

        def piece(shift):
            target = (me_z + shift) % nz
            block = lax.dynamic_slice(
                cut, (target, me_x, 0, 0, 0), (1, 1, share, rows, width)
            ).reshape(share, rows, width)
            return block.transpose(1, 0, 2)

        own = trial_vectors.transpose(1, 0, 2)
        group = own.shape[1]
        compact = own.astype(B16)
        near = {s: piece(s) for s in (1, nz - 1)}
        near, compact = lax.optimization_barrier((near, compact))
        blocks = {s: send_z(near[s], s, nz) for s in near}
        for s in order:
            if s and s not in near:
                blocks[s] = send_z(piece(s), s, nz)
        blocks[0] = piece(0)
        vectors = {s: both_groups(move_z(compact, s, nz), me_x, nx) for s in order}
        gap = energy_gap[:, None, :]
        coupling = None
        for iteration in range(ITERS):
            mixed = None
            gram = None
            for s in order:
                term = jnp.einsum(
                    "lkn,rpn->rlkp", vectors[s], blocks[s], preferred_element_type=F32
                )
                mixed = term if mixed is None else mixed + term
                corr = jnp.einsum(
                    "rkn,rln->kl", vectors[s], vectors[s], preferred_element_type=F32
                )
                gram = corr if gram is None else gram + corr
            lower = jnp.linalg.cholesky(gram)
            inverse = lax.linalg.triangular_solve(
                lower, jnp.eye(gram.shape[0], dtype=F32), left_side=True, lower=True
            )
            diagonal = jnp.eye(rows, dtype=F32)[:, :, None, None]
            fitted = jnp.sum(mixed * diagonal, axis=(0, 1)).astype(B16).astype(F32)
            weights = (2.0 * diagonal * fitted[None, None] - mixed).astype(B16)
            fock = None
            for s in reversed(order):
                part = jnp.einsum(
                    "rlkp,lpn->rkn", weights, blocks[s], preferred_element_type=F32
                )
                mine = lax.dynamic_slice_in_dim(part, me_x * group, group, 1)
                theirs = lax.dynamic_slice_in_dim(part, (1 - me_x) * group, group, 1)
                got = lax.ppermute(theirs.astype(B16), "gx", ring(nx, 1))
                part = mine + got.astype(F32)
                if s:
                    part = move_z(part.astype(B16), -s, nz).astype(F32)
                fock = part if fock is None else fock + part
            fock = fock.astype(B16)
            left, right = lax.split(fock, (group // 2, group - group // 2), axis=1)
            fock = lax.concatenate(
                (butterfly(left, ny, False), butterfly(right, ny, True)), 1
            ).astype(F32)
            everyone = vectors[0]
            sigma = gap * own + fock
            share_of = jnp.einsum(
                "rln,rkn->lk", everyone, sigma.astype(B16), preferred_element_type=F32
            )
            projected = share_of
            parts = [share_of] + [
                lax.ppermute(share_of, "gz", ring(nz, s)) for s in range(1, nz)
            ]
            slots = jnp.stack(parts)
            slots = jnp.take(slots, (me_z - jnp.arange(nz)) % nz, axis=0)
            projected = jnp.sum(slots, axis=0)
            highest = lax.Precision.HIGHEST
            inner = jnp.dot(inverse, projected, precision=highest)
            coupling = jnp.dot(inverse.T, inner, precision=highest)
            spanned = jnp.einsum(
                "rln,lk->rkn", everyone, coupling.astype(B16), preferred_element_type=F32
            )
            own = (spanned - fock) / gap
            if iteration < ITERS - 1:
                compact = own.astype(B16)
                vectors = {s: both_groups(move_z(compact, s, nz), me_x, nx) for s in order}
        return (own.transpose(1, 0, 2), coupling)

    return per_device


def solution(mesh):
    placed = (P("gy", None, "gz"), P("gx", None, "gz"), P(None, "gz"))
    return jax.shard_map(
        make_per_device(mesh.shape["gx"], mesh.shape["gy"], mesh.shape["gz"]),
        mesh=mesh,
        in_specs=placed,
        out_specs=(P("gx", None, "gz"), P(None, "gx")),
        check_vma=False,
    )
```

```python
import jax
import jax.numpy as jnp
from jax import lax
from jax.sharding import PartitionSpec as P

ITERS = 2
B16 = jnp.bfloat16
F32 = jnp.float32


def ring(size, shift):
    return [(i, (i + shift) % size) for i in range(size)]


def send_z(block, shift, size, axis=1):
    shift = shift % size
    if 2 * shift != size:
        return lax.ppermute(block, "gz", ring(size, shift))
    half = block.shape[axis] // 2
    first, second = lax.split(block, (half, block.shape[axis] - half), axis=axis)
    for part_shift in (1, shift - 1):
        if part_shift:
            first = lax.ppermute(first, "gz", ring(size, part_shift))
            second = lax.ppermute(second, "gz", ring(size, -part_shift))
    return lax.concatenate((first, second), axis)


def move_z(block, shift, size):
    shift = shift % size
    return lax.ppermute(block, "gz", ring(size, shift)) if shift else block


def butterfly(block, size, descending):
    bits = [1 << b for b in range(size.bit_length() - 1)]
    for bit in reversed(bits) if descending else bits:
        other = lax.ppermute(block, "gy", [(i, i ^ bit) for i in range(size)])
        block = (block.astype(F32) + other.astype(F32)).astype(B16)
    return block


def both_groups(block, me, size_x):
    other = lax.ppermute(block, "gx", ring(size_x, 1))
    first = jnp.where(me == 0, block, other)
    second = jnp.where(me == 0, other, block)
    return lax.concatenate((first, second), 1)


def make_per_device(nx, ny, nz):
    order = sorted(range(nz), key=lambda s: min(s, nz - s))

    def per_device(factors, trial_vectors, energy_gap):
        me_x, me_z = lax.axis_index("gx"), lax.axis_index("gz")
        aux, rows, width = factors.shape
        share = aux // (nx * nz)
        cut = factors.reshape(nz, nx, share, rows, width)

        def piece(shift):
            target = (me_z + shift) % nz
            block = lax.dynamic_slice(
                cut, (target, me_x, 0, 0, 0), (1, 1, share, rows, width)
            ).reshape(share, rows, width)
            return block.transpose(1, 0, 2)

        own = trial_vectors.transpose(1, 0, 2)
        group = own.shape[1]
        compact = own.astype(B16)
        near = {s: piece(s) for s in reversed(order) if s}
        near, compact = lax.optimization_barrier((near, compact))
        blocks = {s: send_z(near[s], s, nz) for s in near}
        for s in order:
            if s and s not in near:
                blocks[s] = send_z(piece(s), s, nz)
        blocks[0] = piece(0)
        vectors = {s: both_groups(move_z(compact, s, nz), me_x, nx) for s in order}
        gap = energy_gap[:, None, :]
        coupling = None
        for iteration in range(ITERS):
            mixed = None
            gram = None
            for s in order:
                term = jnp.einsum(
                    "lkn,rpn->rlkp", vectors[s], blocks[s], preferred_element_type=F32
                )
                mixed = term if mixed is None else mixed + term
                corr = jnp.einsum(
                    "rkn,rln->kl", vectors[s], vectors[s], preferred_element_type=F32
                )
                gram = corr if gram is None else gram + corr
            lower = jnp.linalg.cholesky(gram)
            inverse = lax.linalg.triangular_solve(
                lower, jnp.eye(gram.shape[0], dtype=F32), left_side=True, lower=True
            )
            diagonal = jnp.eye(rows, dtype=F32)[:, :, None, None]
            fitted = jnp.sum(mixed * diagonal, axis=(0, 1)).astype(B16).astype(F32)
            weights = (2.0 * diagonal * fitted[None, None] - mixed).astype(B16)
            fock = None
            for s in reversed(order):
                part = jnp.einsum(
                    "rlkp,lpn->rkn", weights, blocks[s], preferred_element_type=F32
                )
                mine = lax.dynamic_slice_in_dim(part, me_x * group, group, 1)
                theirs = lax.dynamic_slice_in_dim(part, (1 - me_x) * group, group, 1)
                got = lax.ppermute(theirs.astype(B16), "gx", ring(nx, 1))
                part = mine + got.astype(F32)
                if s:
                    part = move_z(part.astype(B16), -s, nz).astype(F32)
                fock = part if fock is None else fock + part
            fock = fock.astype(B16)
            left, right = lax.split(fock, (group // 2, group - group // 2), axis=1)
            fock = lax.concatenate(
                (butterfly(left, ny, False), butterfly(right, ny, True)), 1
            ).astype(F32)
            everyone = vectors[0]
            sigma = gap * own + fock
            share_of = jnp.einsum(
                "rln,rkn->lk", everyone, sigma.astype(B16), preferred_element_type=F32
            )
            projected = share_of
            parts = [share_of] + [
                lax.ppermute(share_of, "gz", ring(nz, s)) for s in range(1, nz)
            ]
            slots = jnp.stack(parts)
            slots = jnp.take(slots, (me_z - jnp.arange(nz)) % nz, axis=0)
            projected = jnp.sum(slots, axis=0)
            highest = lax.Precision.HIGHEST
            inner = jnp.dot(inverse, projected, precision=highest)
            coupling = jnp.dot(inverse.T, inner, precision=highest)
            spanned = jnp.einsum(
                "rln,lk->rkn", everyone, coupling.astype(B16), preferred_element_type=F32
            )
            own = (spanned - fock) / gap
            if iteration < ITERS - 1:
                compact = own.astype(B16)
                vectors = {s: both_groups(move_z(compact, s, nz), me_x, nx) for s in order}
        return (own.transpose(1, 0, 2), coupling)

    return per_device


def solution(mesh):
    placed = (P("gy", None, "gz"), P("gx", None, "gz"), P(None, "gz"))
    return jax.shard_map(
        make_per_device(mesh.shape["gx"], mesh.shape["gy"], mesh.shape["gz"]),
        mesh=mesh,
        in_specs=placed,
        out_specs=(P("gx", None, "gz"), P(None, "gx")),
        check_vma=False,
    )
```
